32 devices in a mesh: gx: 4 (over x, core), gy: 2 (over y), gz: 4 (over z).
Axes of the slice: x: 2, y: 2, z: 4, core: 2. Of those that a mesh axis runs over, the one named last changes fastest.
Arguments:
- fields: float32 [32, 32, 16, 512], P(None, 'gx', 'gy', 'gz'), may hold values from -8 to 8
- strength: float32 [32], replicated, may hold values from 0.3 to 1
Outputs:
- filtered: float32 [32, 32, 16, 512], P(None, 'gx', 'gy', 'gz')
The draws below stay inside these ranges and needn't reach their ends.
All inputs are finite; a program needn't handle non-finite values.
Results may differ from the reference program's by a relative error of at most 0.00002.
Values sent between devices are 32-bit elements; how exact they have to be, the bound alone decides.
A program may use at most 64 MiB of HBM per device.

```python
import math
import jax
import jax.numpy as jnp
from jax import lax

SPECIES = 32
NX = 32
NY = 16
NZ = 512


def steps_of(own_key, extent, shards, smallest, top_value):
    def one(axis_at, shards_of):
        draws = jax.random.uniform(jax.random.fold_in(jax.random.fold_in(own_key, 6), axis_at), (shards_of,), jnp.float32, smallest / len(shards), top_value / len(shards))
        return jnp.repeat(jnp.exp(draws), extent[axis_at] // shards_of).reshape((-1,) + (1,) * (len(extent) - axis_at - 1))

    gain = one(*shards[0])
    for cut in shards[1:]:
        gain = gain * one(*cut)
    return gain


def scatter_about(own_key, shape, scale, reach, split=(), kind=jnp.bfloat16):
    values = jax.random.normal(own_key, shape, jnp.float32) * scale
    if len(split) > 0:
        values = steps_of(own_key, shape, split, -0.22, 0.18) * values
    return jnp.clip(values, min=-reach, max=reach).astype(kind)


def setup_inputs(seed: int = 0) -> dict:
    key_of = jax.random.split(jax.random.key(seed), 3)
    fields = scatter_about(key_of[0], (SPECIES, NX, NY, NZ), 1.0, 8.0, ((1, 4), (2, 2), (3, 4)), jnp.float32)
    strength = jnp.clip(jnp.exp(jax.random.uniform(key_of[1], (SPECIES,), jnp.float32, math.log(0.3), math.log(1.0))), 0.3, 1.0)
    return {"fields": fields, "strength": strength}


filter_weights = [1.0, -10.0, 45.0, -120.0, 210.0, -252.0, 210.0, -120.0, 45.0, -10.0, 1.0]


def tenth_difference(field, axis):
    total = jnp.zeros(field.shape, jnp.float32)
    for index in range(11):
        total = total + filter_weights[index] * jnp.roll(field, 5 - index, axis)
    return total


def filter_species(packed):
    field, scale = packed
    summed = tenth_difference(field, 0) + tenth_difference(field, 1) + tenth_difference(field, 2)
    return field + (scale / 1024.0) * summed


def reference(fields, strength):
    return lax.map(filter_species, (fields, strength))
```

```python
import functools
import jax
import jax.numpy as jnp
from jax import lax
from jax.experimental import pallas as pl
from jax.experimental.pallas import tpu as pltpu
from jax.sharding import PartitionSpec as P

MESH = pl.DeviceIdType.MESH
REACH = 5
SLOT = 8
WEIGHTS = [-252.0, 210.0, -120.0, 45.0, -10.0, 1.0]
CUTS = (4, 4, 4, 4, 4, 4, 4, 2, 2)


def weight_of(offset):
    return WEIGHTS[abs(offset)] if abs(offset) <= REACH else 0.0


def row_weights(rows, lanes, roll, bases):
    row = lax.broadcasted_iota(jnp.int32, (rows, lanes), 0)
    out = jnp.zeros((rows, lanes), jnp.float32)
    for i in range(rows):
        value = sum(weight_of((i + roll) % rows + base - i) for base in bases)
        if value:
            out = jnp.where(row == i, value, out)
    return out


def rolled_rows(block, roll):
    rows = block.shape[1]
    return block if roll == 0 else pltpu.roll(block, rows - roll, 1)


def rows_sum(block, weights):
    total = None
    for roll, weight in enumerate(weights):
        term = weight[None] * rolled_rows(block, roll)
        total = term if total is None else total + term
    return total


def kernel(nx, ny, nz, cuts, fields, strength, out, u, acc, done, xl, xr, ys, packed, landed,
           in_sem, out_sem, x_send, x_recv, y_send, y_recv, z_send, z_recv):
    species, cx, cy, cz = u.shape
    groups = cz // SLOT
    rows_packed = packed.shape[1]
    px, py, pz = lax.axis_index("gx"), lax.axis_index("gy"), lax.axis_index("gz")
    x_left, x_right = lax.rem(px + nx - 1, nx), lax.rem(px + 1, nx)
    y_left, y_right = lax.rem(py + ny - 1, ny), lax.rem(py + 1, ny)
    z_left, z_right = lax.rem(pz + nz - 1, nz), lax.rem(pz + 1, nz)
    y_peers = [y_right] if ny == 2 else [y_right, y_left]

    barrier = pltpu.get_barrier_semaphore()
    near = [(x_left, py, pz), (x_right, py, pz), (px, py, z_left), (px, py, z_right)]
    near += [(px, peer, pz) for peer in y_peers]
    for peer in near:
        pl.semaphore_signal(barrier, inc=1, device_id=peer, device_id_type=MESH)

    spans = []
    begin = 0
    for size in cuts:
        spans.append((begin, size))
        begin += size
    loads = []
    for k, (begin, size) in enumerate(spans):
        part = pl.ds(begin, size)
        loads.append(pltpu.make_async_copy(fields.at[part], u.at[part], in_sem.at[k]))
        loads[-1].start()
    for load in loads:
        load.wait()

    lane = lax.broadcasted_iota(jnp.int32, (cx, cy, cz), 2)
    slot = lane // SLOT
    for p in range(rows_packed):
        first = p * groups
        here = min(groups, species - first)

        def pack(g, carry):
            head, tail = carry
            v = u[first + g]
            mine = slot == g
            head = jnp.where(mine, pltpu.roll(v, g * SLOT, 2), head)
            tail = jnp.where(mine, pltpu.roll(v, lax.rem((g + 1) * SLOT, cz), 2), tail)
            return head, tail

        zero = jnp.zeros((cx, cy, cz), jnp.float32)
        head, tail = lax.fori_loop(0, here, pack, (zero, zero))
        packed[0, p] = head
        packed[1, p] = tail

    pl.semaphore_wait(barrier, len(near))

    y_copies, x_copies = [], []
    for k, (begin, size) in enumerate(spans):
        part = pl.ds(begin, size)
        row = []
        for side, peer in enumerate(y_peers):
            row.append(pltpu.make_async_remote_copy(
                src_ref=u.at[part], dst_ref=ys.at[side, part],
                send_sem=y_send.at[side, k], recv_sem=y_recv.at[side, k],
                device_id=(px, peer, pz), device_id_type=MESH))
        y_copies.append(row)
        x_copies.append([
            pltpu.make_async_remote_copy(
                src_ref=u.at[part, pl.ds(cx - REACH, REACH)], dst_ref=xl.at[part],
                send_sem=x_send.at[0, k], recv_sem=x_recv.at[0, k],
                device_id=(x_right, py, pz), device_id_type=MESH),
            pltpu.make_async_remote_copy(
                src_ref=u.at[part, pl.ds(0, REACH)], dst_ref=xr.at[part],
                send_sem=x_send.at[1, k], recv_sem=x_recv.at[1, k],
                device_id=(x_left, py, pz), device_id_type=MESH),
        ])
    z_copies = [
        pltpu.make_async_remote_copy(
            src_ref=packed.at[side], dst_ref=landed.at[side],
            send_sem=z_send.at[side], recv_sem=z_recv.at[side],
            device_id=(px, py, peer), device_id_type=MESH)
        for side, peer in enumerate((z_left, z_right))
    ]
    for copy in y_copies[0] + x_copies[0] + z_copies:
        copy.start()
    for k in range(1, len(spans)):
        for copy in y_copies[k] + x_copies[k]:
            copy.start()

    own = [row_weights(cy, cz, r, (0,)) for r in range(cy)]
    if ny == 2:
        remote = [[row_weights(cy, cz, r, (cy, -cy)) for r in range(cy)]]
    else:
        remote = [[row_weights(cy, cz, r, (base,)) for r in range(cy)] for base in (-cy, cy)]

    for copy in z_copies:
        copy.wait()

    def along_z(s, _):
        v = u[s]
        p, g = s // groups, lax.rem(s, groups)
        after = pltpu.roll(landed[0, p], lax.rem(cz - g * SLOT, cz), 2)
        before = pltpu.roll(landed[1, p], cz - (g + 1) * SLOT, 2)
        total = (2.0 * WEIGHTS[0]) * v
        for d in range(1, REACH + 1):
            up = pltpu.roll(jnp.where(lane < d, after, v), cz - d, 2)
            down = pltpu.roll(jnp.where(lane >= cz - d, before, v), d, 2)
            total = total + WEIGHTS[d] * (up + down)
        acc[s] = total + rows_sum(v, own)
        return 0

    lax.fori_loop(0, species, along_z, 0)

    def along_x(s, _):
        cells = [xl[s, i] for i in range(REACH)] + [u[s, i] for i in range(cx)]
        cells += [xr[s, i] for i in range(REACH)]
        for i in range(cx):
            total = acc[s, i]
            for d in range(1, REACH + 1):
                total = total + WEIGHTS[d] * (cells[REACH + i - d] + cells[REACH + i + d])
            acc[s, i] = total
        return 0

    def along_y(s, _):
        total = acc[s]
        for side, weights in enumerate(remote):
            total = total + rows_sum(ys[side, s], weights)
        done[s] = u[s] + (strength[s] * (1.0 / 1024.0)) * total
        return 0

    stores = []
    for k, (begin, size) in enumerate(spans):
        part = pl.ds(begin, size)
        for copy in x_copies[k]:
            copy.wait_recv()
        lax.fori_loop(begin, begin + size, along_x, 0)
        for copy in y_copies[k]:
            copy.wait_recv()
        lax.fori_loop(begin, begin + size, along_y, 0)
        stores.append(pltpu.make_async_copy(done.at[part], out.at[part], out_sem.at[k]))
        stores[-1].start()
    for k in range(len(spans)):
        for copy in y_copies[k] + x_copies[k]:
            copy.wait_send()
    for store in stores:
        store.wait()


def local(nx, ny, nz, fields, strength):
    species, cx, cy, cz = fields.shape
    cuts = CUTS if sum(CUTS) == species else (1,) * species
    pieces = len(cuts)
    sides = 1 if ny == 2 else 2
    groups = cz // SLOT
    rows_packed = -(-species // groups)
    block = (species, cx, cy, cz)
    dma = pltpu.SemaphoreType.DMA
    return pl.pallas_call(
        functools.partial(kernel, nx, ny, nz, cuts),
        out_shape=jax.ShapeDtypeStruct(block, jnp.float32),
        in_specs=[pl.BlockSpec(memory_space=pl.ANY), pl.BlockSpec(memory_space=pltpu.SMEM)],
        out_specs=pl.BlockSpec(memory_space=pl.ANY),
        scratch_shapes=[
            pltpu.VMEM(block, jnp.float32),
            pltpu.VMEM(block, jnp.float32),
            pltpu.VMEM(block, jnp.float32),
            pltpu.VMEM((species, REACH, cy, cz), jnp.float32),
            pltpu.VMEM((species, REACH, cy, cz), jnp.float32),
            pltpu.VMEM((sides,) + block, jnp.float32),
            pltpu.VMEM((2, rows_packed, cx, cy, cz), jnp.float32),
            pltpu.VMEM((2, rows_packed, cx, cy, cz), jnp.float32),
            dma((pieces,)),
            dma((pieces,)),
            dma((2, pieces)),
            dma((2, pieces)),
            dma((sides, pieces)),
            dma((sides, pieces)),
            dma((2,)),
            dma((2,)),
        ],
        compiler_params=pltpu.CompilerParams(collective_id=0, has_side_effects=True),
        name="filter_pass",
    )(fields, strength)


def solution(mesh):
    sizes = mesh.shape
    return jax.shard_map(
        functools.partial(local, sizes["gx"], sizes["gy"], sizes["gz"]),
        mesh=mesh,
        in_specs=(P(None, "gx", "gy", "gz"), P()),
        out_specs=P(None, "gx", "gy", "gz"),
        check_vma=False,
    )
```

```python
import functools
import jax
import jax.numpy as jnp
from jax import lax
from jax.experimental import pallas as pl
from jax.experimental.pallas import tpu as pltpu
from jax.sharding import PartitionSpec as P

MESH = pl.DeviceIdType.MESH
REACH = 5
SLOT = 8
WEIGHTS = [-252.0, 210.0, -120.0, 45.0, -10.0, 1.0]
CUTS = (4, 4, 4, 4, 4, 4, 4, 2, 2)


def weight_of(offset):
    return WEIGHTS[abs(offset)] if abs(offset) <= REACH else 0.0


def row_weights(rows, lanes, roll, bases):
    row = lax.broadcasted_iota(jnp.int32, (rows, lanes), 0)
    out = jnp.zeros((rows, lanes), jnp.float32)
    for i in range(rows):
        value = sum(weight_of((i + roll) % rows + base - i) for base in bases)
        if value:
            out = jnp.where(row == i, value, out)
    return out


def rolled_rows(block, roll):
    rows = block.shape[1]
    return block if roll == 0 else pltpu.roll(block, rows - roll, 1)


def rows_sum(block, weights):
    total = None
    for roll, weight in enumerate(weights):
        term = weight[None] * rolled_rows(block, roll)
        total = term if total is None else total + term
    return total


def kernel(nx, ny, nz, cuts, fields, strength, out, u, acc, xl, xr, ys, packed, landed,
           in_sem, x_send, x_recv, y_send, y_recv, z_send, z_recv, rising, falling):
    species, cx, cy, cz = u.shape
    groups = cz // SLOT
    rows_packed = packed.shape[1]
    px, py, pz = lax.axis_index("gx"), lax.axis_index("gy"), lax.axis_index("gz")
    x_left, x_right = lax.rem(px + nx - 1, nx), lax.rem(px + 1, nx)
    y_left, y_right = lax.rem(py + ny - 1, ny), lax.rem(py + 1, ny)
    z_left, z_right = lax.rem(pz + nz - 1, nz), lax.rem(pz + 1, nz)
    y_peers = [y_right] if ny == 2 else [y_right, y_left]

    barrier = pltpu.get_barrier_semaphore()
    near = [(x_left, py, pz), (x_right, py, pz)] + [(px, peer, pz) for peer in y_peers]
    for peer in near:
        pl.semaphore_signal(barrier, inc=1, device_id=peer, device_id_type=MESH)

    @pl.when(pz > 0)
    def _():
        pl.semaphore_signal(barrier, inc=1, device_id=(px, py, z_left), device_id_type=MESH)

    @pl.when(pz < nz - 1)
    def _():
        pl.semaphore_signal(barrier, inc=1, device_id=(px, py, z_right), device_id_type=MESH)

    spans = []
    begin = 0
    for size in cuts:
        spans.append((begin, size))
        begin += size
    loads = []
    for k, (begin, size) in enumerate(spans):
        part = pl.ds(begin, size)
        loads.append(pltpu.make_async_copy(fields.at[part], u.at[part], in_sem.at[k]))
        loads[-1].start()
    ends = (pz > 0).astype(jnp.int32) + (pz < nz - 1).astype(jnp.int32)
    pl.semaphore_wait(barrier, len(near) + ends)

    y_copies, x_copies = [], []
    for k, (begin, size) in enumerate(spans):
        part = pl.ds(begin, size)
        row = []
        for side, peer in enumerate(y_peers):
            row.append(pltpu.make_async_remote_copy(
                src_ref=fields.at[part], dst_ref=ys.at[side, part],
                send_sem=y_send.at[side, k], recv_sem=y_recv.at[side, k],
                device_id=(px, peer, pz), device_id_type=MESH))
        y_copies.append(row)
        x_copies.append([
            pltpu.make_async_remote_copy(
                src_ref=u.at[part, pl.ds(cx - REACH, REACH)], dst_ref=xl.at[part],
                send_sem=x_send.at[0, k], recv_sem=x_recv.at[0, k],
                device_id=(x_right, py, pz), device_id_type=MESH),
            pltpu.make_async_remote_copy(
                src_ref=u.at[part, pl.ds(0, REACH)], dst_ref=xr.at[part],
                send_sem=x_send.at[1, k], recv_sem=x_recv.at[1, k],
                device_id=(x_left, py, pz), device_id_type=MESH),
        ])
    for row in y_copies:
        for copy in row:
            copy.start()
    for load, row in zip(loads, x_copies):
        load.wait()
        for copy in row:
            copy.start()

    lane = lax.broadcasted_iota(jnp.int32, (cx, cy, cz), 2)
    slot = lane // SLOT
    for p in range(rows_packed):
        first = p * groups
        here = min(groups, species - first)

        def pack(g, carry):
            head, tail = carry
            v = u[first + g]
            mine = slot == g
            head = jnp.where(mine, pltpu.roll(v, g * SLOT, 2), head)
            tail = jnp.where(mine, pltpu.roll(v, lax.rem((g + 1) * SLOT, cz), 2), tail)
            return head, tail

        zero = jnp.zeros((cx, cy, cz), jnp.float32)
        head, tail = lax.fori_loop(0, here, pack, (zero, zero))
        packed[0, p] = head
        packed[1, p] = tail

    inner = jnp.logical_and(pz > 0, pz < nz - 1)
    to_left, to_right = (px, py, z_left), (px, py, z_right)

    @pl.when(pz == 0)
    def _():
        pl.semaphore_signal(rising, inc=1, device_id=to_right, device_id_type=MESH)

    @pl.when(pz == nz - 1)
    def _():
        pl.semaphore_signal(falling, inc=1, device_id=to_left, device_id_type=MESH)

    @pl.when(pz > 0)
    def _():
        pl.semaphore_wait(rising, 1)

    @pl.when(inner)
    def _():
        pl.semaphore_signal(rising, inc=1, device_id=to_right, device_id_type=MESH)

    @pl.when(pz < nz - 1)
    def _():
        pl.semaphore_wait(falling, 1)

    @pl.when(inner)
    def _():
        pl.semaphore_signal(falling, inc=1, device_id=to_left, device_id_type=MESH)

    z_copies = [
        pltpu.make_async_remote_copy(
            src_ref=packed.at[side], dst_ref=landed.at[side],
            send_sem=z_send.at[side], recv_sem=z_recv.at[side],
            device_id=(px, py, peer), device_id_type=MESH)
        for side, peer in enumerate((z_left, z_right))
    ]
    for copy in z_copies:
        copy.start()

    own = [row_weights(cy, cz, r, (0,)) for r in range(cy)]
    if ny == 2:
        remote = [[row_weights(cy, cz, r, (cy, -cy)) for r in range(cy)]]
    else:
        remote = [[row_weights(cy, cz, r, (base,)) for r in range(cy)] for base in (-cy, cy)]

    for copy in z_copies:
        copy.wait()

    def along_z(s, _):
        v = u[s]
        p, g = s // groups, lax.rem(s, groups)
        after = pltpu.roll(landed[0, p], lax.rem(cz - g * SLOT, cz), 2)
        before = pltpu.roll(landed[1, p], cz - (g + 1) * SLOT, 2)
        total = (2.0 * WEIGHTS[0]) * v
        for d in range(1, REACH + 1):
            up = pltpu.roll(jnp.where(lane < d, after, v), cz - d, 2)
            down = pltpu.roll(jnp.where(lane >= cz - d, before, v), d, 2)
            total = total + WEIGHTS[d] * (up + down)
        acc[s] = total + rows_sum(v, own)
        return 0

    lax.fori_loop(0, species, along_z, 0)

    def along_x(s, _):
        cells = [xl[s, i] for i in range(REACH)] + [u[s, i] for i in range(cx)]
        cells += [xr[s, i] for i in range(REACH)]
        for i in range(cx):
            total = acc[s, i]
            for d in range(1, REACH + 1):
                total = total + WEIGHTS[d] * (cells[REACH + i - d] + cells[REACH + i + d])
            acc[s, i] = total
        return 0

    def along_y(s, _):
        total = acc[s]
        for side, weights in enumerate(remote):
            total = total + rows_sum(ys[side, s], weights)
        out[s] = u[s] + (strength[s] * (1.0 / 1024.0)) * total
        return 0

    for k, (begin, size) in enumerate(spans):
        part = pl.ds(begin, size)
        for copy in x_copies[k]:
            copy.wait_recv()
        lax.fori_loop(begin, begin + size, along_x, 0)
        for copy in y_copies[k]:
            copy.wait_recv()
        lax.fori_loop(begin, begin + size, along_y, 0)
    for k in range(len(spans)):
        for copy in y_copies[k] + x_copies[k]:
            copy.wait_send()


def local(nx, ny, nz, fields, strength):
    species, cx, cy, cz = fields.shape
    cuts = CUTS if sum(CUTS) == species else (1,) * species
    pieces = len(cuts)
    sides = 1 if ny == 2 else 2
    groups = cz // SLOT
    rows_packed = -(-species // groups)
    block = (species, cx, cy, cz)
    dma = pltpu.SemaphoreType.DMA
    return pl.pallas_call(
        functools.partial(kernel, nx, ny, nz, cuts),
        out_shape=pltpu.VMEM(block, jnp.float32),
        in_specs=[pl.BlockSpec(memory_space=pltpu.HBM), pl.BlockSpec(memory_space=pltpu.SMEM)],
        out_specs=pl.BlockSpec(memory_space=pltpu.VMEM),
        scratch_shapes=[
            pltpu.VMEM(block, jnp.float32),
            pltpu.VMEM(block, jnp.float32),
            pltpu.VMEM((species, REACH, cy, cz), jnp.float32),
            pltpu.VMEM((species, REACH, cy, cz), jnp.float32),
            pltpu.VMEM((sides,) + block, jnp.float32),
            pltpu.VMEM((2, rows_packed, cx, cy, cz), jnp.float32),
            pltpu.VMEM((2, rows_packed, cx, cy, cz), jnp.float32),
            dma((pieces,)),
            dma((2, pieces)),
            dma((2, pieces)),
            dma((sides, pieces)),
            dma((sides, pieces)),
            dma((2,)),
            dma((2,)),
            pltpu.SemaphoreType.REGULAR,
            pltpu.SemaphoreType.REGULAR,
        ],
        compiler_params=pltpu.CompilerParams(collective_id=0, has_side_effects=True, vmem_limit_bytes=56 * 1024 * 1024),
        name="filter_pass",
    )(fields, strength)


def solution(mesh):
    sizes = mesh.shape
    return jax.shard_map(
        functools.partial(local, sizes["gx"], sizes["gy"], sizes["gz"]),
        mesh=mesh,
        in_specs=(P(None, "gx", "gy", "gz"), P()),
        out_specs=P(None, "gx", "gy", "gz"),
        check_vma=False,
    )
```

```python
import functools
import jax
import jax.numpy as jnp
from jax import lax
from jax.experimental import pallas as pl
from jax.experimental.pallas import tpu as pltpu
from jax.sharding import PartitionSpec as P

MESH = pl.DeviceIdType.MESH
REACH = 5
SLOT = 8
WEIGHTS = [-252.0, 210.0, -120.0, 45.0, -10.0, 1.0]
CUTS = (4, 4, 4, 4, 4, 4, 4, 2, 2)


def weight_of(offset):
    return WEIGHTS[abs(offset)] if abs(offset) <= REACH else 0.0


def row_weights(rows, lanes, roll, bases):
    row = lax.broadcasted_iota(jnp.int32, (rows, lanes), 0)
    out = jnp.zeros((rows, lanes), jnp.float32)
    for i in range(rows):
        value = sum(weight_of((i + roll) % rows + base - i) for base in bases)
        if value:
            out = jnp.where(row == i, value, out)
    return out


def rolled_rows(block, roll):
    rows = block.shape[1]
    return block if roll == 0 else pltpu.roll(block, rows - roll, 1)


def rows_sum(block, weights):
    total = None
    for roll, weight in enumerate(weights):
        term = weight[None] * rolled_rows(block, roll)
        total = term if total is None else total + term
    return total


def kernel(nx, ny, nz, cuts, fields, strength, out, u, acc, xl, xr, ys, packed, landed,
           in_sem, x_send, x_recv, y_send, y_recv, z_send, z_recv, answers):
    species, cx, cy, cz = u.shape
    groups = cz // SLOT
    rows_packed = packed.shape[1]
    px, py, pz = lax.axis_index("gx"), lax.axis_index("gy"), lax.axis_index("gz")
    x_left, x_right = lax.rem(px + nx - 1, nx), lax.rem(px + 1, nx)
    y_left, y_right = lax.rem(py + ny - 1, ny), lax.rem(py + 1, ny)
    z_left, z_right = lax.rem(pz + nz - 1, nz), lax.rem(pz + 1, nz)
    y_peers = [y_right] if ny == 2 else [y_right, y_left]

    barrier = pltpu.get_barrier_semaphore()
    to_left, to_right = (px, py, z_left), (px, py, z_right)
    left_x, right_x = (x_left, py, pz), (x_right, py, pz)
    first_x, last_x, first_z, last_z = px == 0, px == nx - 1, pz == 0, pz == nz - 1

    def tell(semaphore, peer):
        pl.semaphore_signal(semaphore, inc=1, device_id=peer, device_id_type=MESH)

    for peer in y_peers:
        tell(barrier, (px, peer, pz))
    pl.when(px < nx - 1)(lambda: tell(barrier, right_x))
    pl.when(first_x)(lambda: tell(barrier, left_x))
    pl.when(pz < nz - 1)(lambda: tell(barrier, to_right))

    spans = []
    begin = 0
    for size in cuts:
        spans.append((begin, size))
        begin += size
    loads = []
    for k, (begin, size) in enumerate(spans):
        part = pl.ds(begin, size)
        loads.append(pltpu.make_async_copy(fields.at[part], u.at[part], in_sem.at[k]))
        loads[-1].start()
    greeters = sum(c.astype(jnp.int32) for c in (px > 0, last_x, pz > 0))
    pl.semaphore_wait(barrier, len(y_peers) + greeters)

    y_copies, x_copies = [], []
    for k, (begin, size) in enumerate(spans):
        part = pl.ds(begin, size)
        row = []
        for side, peer in enumerate(y_peers):
            row.append(pltpu.make_async_remote_copy(
                src_ref=fields.at[part], dst_ref=ys.at[side, part],
                send_sem=y_send.at[side, k], recv_sem=y_recv.at[side, k],
                device_id=(px, peer, pz), device_id_type=MESH))
        y_copies.append(row)
        x_copies.append([
            pltpu.make_async_remote_copy(
                src_ref=u.at[part, pl.ds(cx - REACH, REACH)], dst_ref=xl.at[part],
                send_sem=x_send.at[0, k], recv_sem=x_recv.at[0, k],
                device_id=(x_right, py, pz), device_id_type=MESH),
            pltpu.make_async_remote_copy(
                src_ref=u.at[part, pl.ds(0, REACH)], dst_ref=xr.at[part],
                send_sem=x_send.at[1, k], recv_sem=x_recv.at[1, k],
                device_id=(x_left, py, pz), device_id_type=MESH),
        ])
    for row in y_copies:
        for copy in row:
            copy.start()
    pl.when(px > 0)(lambda: tell(answers.at[0], left_x))
    pl.when(last_x)(lambda: tell(answers.at[1], right_x))
    pl.when(last_z)(lambda: tell(answers.at[2], to_left))
    for load in loads:
        load.wait()
    pl.when(px < nx - 1)(lambda: pl.semaphore_wait(answers.at[0], 1))
    pl.when(first_x)(lambda: pl.semaphore_wait(answers.at[1], 1))
    for row in x_copies:
        for copy in row:
            copy.start()

    lane = lax.broadcasted_iota(jnp.int32, (cx, cy, cz), 2)
    slot = lane // SLOT
    for p in range(rows_packed):
        first = p * groups
        here = min(groups, species - first)

        def pack(g, carry):
            head, tail = carry
            v = u[first + g]
            mine = slot == g
            head = jnp.where(mine, pltpu.roll(v, g * SLOT, 2), head)
            tail = jnp.where(mine, pltpu.roll(v, lax.rem((g + 1) * SLOT, cz), 2), tail)
            return head, tail

        zero = jnp.zeros((cx, cy, cz), jnp.float32)
        head, tail = lax.fori_loop(0, here, pack, (zero, zero))
        packed[0, p] = head
        packed[1, p] = tail

    pl.when(pz < nz - 1)(lambda: pl.semaphore_wait(answers.at[2], 1))
    pl.when(jnp.logical_and(pz > 0, pz < nz - 1))(lambda: tell(answers.at[2], to_left))
    pl.when(first_z)(lambda: tell(answers.at[3], to_left))
    pl.when(last_z)(lambda: pl.semaphore_wait(answers.at[3], 1))
    z_copies = [
        pltpu.make_async_remote_copy(
            src_ref=packed.at[side], dst_ref=landed.at[side],
            send_sem=z_send.at[side], recv_sem=z_recv.at[side],
            device_id=(px, py, peer), device_id_type=MESH)
        for side, peer in enumerate((z_left, z_right))
    ]
    for copy in z_copies:
        copy.start()

    own = [row_weights(cy, cz, r, (0,)) for r in range(cy)]
    if ny == 2:
        remote = [[row_weights(cy, cz, r, (cy, -cy)) for r in range(cy)]]
    else:
        remote = [[row_weights(cy, cz, r, (base,)) for r in range(cy)] for base in (-cy, cy)]

    for copy in z_copies:
        copy.wait()

    def along_z(s, _):
        v = u[s]
        p, g = s // groups, lax.rem(s, groups)
        after = pltpu.roll(landed[0, p], lax.rem(cz - g * SLOT, cz), 2)
        before = pltpu.roll(landed[1, p], cz - (g + 1) * SLOT, 2)
        total = (2.0 * WEIGHTS[0]) * v
        for d in range(1, REACH + 1):
            up = pltpu.roll(jnp.where(lane < d, after, v), cz - d, 2)
            down = pltpu.roll(jnp.where(lane >= cz - d, before, v), d, 2)
            total = total + WEIGHTS[d] * (up + down)
        acc[s] = total + rows_sum(v, own)
        return 0

    lax.fori_loop(0, species, along_z, 0)

    def along_x(s, _):
        cells = [xl[s, i] for i in range(REACH)] + [u[s, i] for i in range(cx)]
        cells += [xr[s, i] for i in range(REACH)]
        for i in range(cx):
            total = acc[s, i]
            for d in range(1, REACH + 1):
                total = total + WEIGHTS[d] * (cells[REACH + i - d] + cells[REACH + i + d])
            acc[s, i] = total
        return 0

    def along_y(s, _):
        total = acc[s]
        for side, weights in enumerate(remote):
            total = total + rows_sum(ys[side, s], weights)
        out[s] = u[s] + (strength[s] * (1.0 / 1024.0)) * total
        return 0

    for k, (begin, size) in enumerate(spans):
        part = pl.ds(begin, size)
        for copy in x_copies[k]:
            copy.wait_recv()
        lax.fori_loop(begin, begin + size, along_x, 0)
        for copy in y_copies[k]:
            copy.wait_recv()
        lax.fori_loop(begin, begin + size, along_y, 0)
    for k in range(len(spans)):
        for copy in y_copies[k] + x_copies[k]:
            copy.wait_send()


def local(nx, ny, nz, fields, strength):
    species, cx, cy, cz = fields.shape
    cuts = CUTS if sum(CUTS) == species else (1,) * species
    pieces = len(cuts)
    sides = 1 if ny == 2 else 2
    groups = cz // SLOT
    rows_packed = -(-species // groups)
    block = (species, cx, cy, cz)
    dma = pltpu.SemaphoreType.DMA
    return pl.pallas_call(
        functools.partial(kernel, nx, ny, nz, cuts),
        out_shape=pltpu.VMEM(block, jnp.float32),
        in_specs=[pl.BlockSpec(memory_space=pltpu.HBM), pl.BlockSpec(memory_space=pltpu.SMEM)],
        out_specs=pl.BlockSpec(memory_space=pltpu.VMEM),
        scratch_shapes=[
            pltpu.VMEM(block, jnp.float32),
            pltpu.VMEM(block, jnp.float32),
            pltpu.VMEM((species, REACH, cy, cz), jnp.float32),
            pltpu.VMEM((species, REACH, cy, cz), jnp.float32),
            pltpu.VMEM((sides,) + block, jnp.float32),
            pltpu.VMEM((2, rows_packed, cx, cy, cz), jnp.float32),
            pltpu.VMEM((2, rows_packed, cx, cy, cz), jnp.float32),
            dma((pieces,)),
            dma((2, pieces)),
            dma((2, pieces)),
            dma((sides, pieces)),
            dma((sides, pieces)),
            dma((2,)),
            dma((2,)),
            pltpu.SemaphoreType.REGULAR((4,)),
        ],
        compiler_params=pltpu.CompilerParams(collective_id=0, has_side_effects=True, vmem_limit_bytes=56 * 1024 * 1024),
        name="filter_pass",
    )(fields, strength)


def solution(mesh):
    sizes = mesh.shape
    return jax.shard_map(
        functools.partial(local, sizes["gx"], sizes["gy"], sizes["gz"]),
        mesh=mesh,
        in_specs=(P(None, "gx", "gy", "gz"), P()),
        out_specs=P(None, "gx", "gy", "gz"),
        check_vma=False,
    )
```

```python
import functools
import jax
import jax.numpy as jnp
from jax import lax
from jax.experimental import pallas as pl
from jax.experimental.pallas import tpu as pltpu
from jax.sharding import PartitionSpec as P

MESH = pl.DeviceIdType.MESH
REACH = 5
SLOT = 8
WEIGHTS = [-252.0, 210.0, -120.0, 45.0, -10.0, 1.0]
CUTS = (4, 4, 4, 4, 4, 4, 4, 2, 2)


def weight_of(offset):
    return WEIGHTS[abs(offset)] if abs(offset) <= REACH else 0.0


def row_weights(rows, lanes, roll, bases):
    row = lax.broadcasted_iota(jnp.int32, (rows, lanes), 0)
    out = jnp.zeros((rows, lanes), jnp.float32)
    for i in range(rows):
        value = sum(weight_of((i + roll) % rows + base - i) for base in bases)
        if value:
            out = jnp.where(row == i, value, out)
    return out


def rolled_rows(block, roll):
    rows = block.shape[1]
    return block if roll == 0 else pltpu.roll(block, rows - roll, 1)


def rows_sum(block, weights):
    total = None
    for roll, weight in enumerate(weights):
        term = weight[None] * rolled_rows(block, roll)
        total = term if total is None else total + term
    return total


def kernel(nx, ny, nz, cuts, fields, strength_in, out, strength, u, acc, xl, xr, ys, packed, landed,
           in_sem, x_send, x_recv, y_send, y_recv, z_send, z_recv, answers):
    species, cx, cy, cz = u.shape
    groups = cz // SLOT
    rows_packed = packed.shape[1]
    px, py, pz = lax.axis_index("gx"), lax.axis_index("gy"), lax.axis_index("gz")
    x_left, x_right = lax.rem(px + nx - 1, nx), lax.rem(px + 1, nx)
    y_left, y_right = lax.rem(py + ny - 1, ny), lax.rem(py + 1, ny)
    z_left, z_right = lax.rem(pz + nz - 1, nz), lax.rem(pz + 1, nz)
    y_peers = [y_right] if ny == 2 else [y_right, y_left]

    barrier = pltpu.get_barrier_semaphore()
    to_left, to_right = (px, py, z_left), (px, py, z_right)
    left_x, right_x = (x_left, py, pz), (x_right, py, pz)
    first_x, last_x, first_z, last_z = px == 0, px == nx - 1, pz == 0, pz == nz - 1

    def tell(semaphore, peer):
        pl.semaphore_signal(semaphore, inc=1, device_id=peer, device_id_type=MESH)

    for peer in y_peers:
        tell(barrier, (px, peer, pz))
    pl.when(px < nx - 1)(lambda: tell(barrier, right_x))
    pl.when(first_x)(lambda: tell(barrier, left_x))
    pl.when(pz < nz - 1)(lambda: tell(barrier, to_right))

    spans = []
    begin = 0
    for size in cuts:
        spans.append((begin, size))
        begin += size
    loads = []
    for k, (begin, size) in enumerate(spans):
        part = pl.ds(begin, size)
        loads.append(pltpu.make_async_copy(fields.at[part], u.at[part], in_sem.at[k]))
    greeters = sum(c.astype(jnp.int32) for c in (px > 0, last_x, pz > 0))
    pl.semaphore_wait(barrier, len(y_peers) + greeters)

    y_copies, x_copies = [], []
    for k, (begin, size) in enumerate(spans):
        part = pl.ds(begin, size)
        row = []
        for side, peer in enumerate(y_peers):
            row.append(pltpu.make_async_remote_copy(
                src_ref=fields.at[part], dst_ref=ys.at[side, part],
                send_sem=y_send.at[side, k], recv_sem=y_recv.at[side, k],
                device_id=(px, peer, pz), device_id_type=MESH))
        y_copies.append(row)
        x_copies.append([
            pltpu.make_async_remote_copy(
                src_ref=u.at[part, pl.ds(cx - REACH, REACH)], dst_ref=xl.at[part],
                send_sem=x_send.at[0, k], recv_sem=x_recv.at[0, k],
                device_id=(x_right, py, pz), device_id_type=MESH),
            pltpu.make_async_remote_copy(
                src_ref=u.at[part, pl.ds(0, REACH)], dst_ref=xr.at[part],
                send_sem=x_send.at[1, k], recv_sem=x_recv.at[1, k],
                device_id=(x_left, py, pz), device_id_type=MESH),
        ])
    for row in y_copies:
        for copy in row:
            copy.start()
    gains = pltpu.make_async_copy(strength_in, strength, in_sem.at[len(cuts)])
    gains.start()
    for load in loads:
        load.start()
    pl.when(px > 0)(lambda: tell(answers.at[0], left_x))
    pl.when(last_x)(lambda: tell(answers.at[1], right_x))
    pl.when(last_z)(lambda: tell(answers.at[2], to_left))
    gains.wait()
    for load in loads:
        load.wait()
    pl.when(px < nx - 1)(lambda: pl.semaphore_wait(answers.at[0], 1))
    pl.when(first_x)(lambda: pl.semaphore_wait(answers.at[1], 1))
    for row in x_copies:
        for copy in row:
            copy.start()

    lane = lax.broadcasted_iota(jnp.int32, (cx, cy, cz), 2)
    slot = lane // SLOT
    for p in range(rows_packed):
        first = p * groups
        here = min(groups, species - first)

        def pack(g, carry):
            head, tail = carry
            v = u[first + g]
            mine = slot == g
            head = jnp.where(mine, pltpu.roll(v, g * SLOT, 2), head)
            tail = jnp.where(mine, pltpu.roll(v, lax.rem((g + 1) * SLOT, cz), 2), tail)
            return head, tail

        zero = jnp.zeros((cx, cy, cz), jnp.float32)
        head, tail = lax.fori_loop(0, here, pack, (zero, zero))
        packed[0, p] = head
        packed[1, p] = tail

    pl.when(pz < nz - 1)(lambda: pl.semaphore_wait(answers.at[2], 1))
    pl.when(jnp.logical_and(pz > 0, pz < nz - 1))(lambda: tell(answers.at[2], to_left))
    pl.when(first_z)(lambda: tell(answers.at[3], to_left))
    pl.when(last_z)(lambda: pl.semaphore_wait(answers.at[3], 1))
    z_copies = [
        pltpu.make_async_remote_copy(
            src_ref=packed.at[side], dst_ref=landed.at[side],
            send_sem=z_send.at[side], recv_sem=z_recv.at[side],
            device_id=(px, py, peer), device_id_type=MESH)
        for side, peer in enumerate((z_left, z_right))
    ]
    for copy in z_copies:
        copy.start()

    own = [row_weights(cy, cz, r, (0,)) for r in range(cy)]
    if ny == 2:
        remote = [[row_weights(cy, cz, r, (cy, -cy)) for r in range(cy)]]
    else:
        remote = [[row_weights(cy, cz, r, (base,)) for r in range(cy)] for base in (-cy, cy)]

    for copy in z_copies:
        copy.wait()

    def along_z(s, _):
        v = u[s]
        p, g = s // groups, lax.rem(s, groups)
        after = pltpu.roll(landed[0, p], lax.rem(cz - g * SLOT, cz), 2)
        before = pltpu.roll(landed[1, p], cz - (g + 1) * SLOT, 2)
        total = (2.0 * WEIGHTS[0]) * v
        for d in range(1, REACH + 1):
            up = pltpu.roll(jnp.where(lane < d, after, v), cz - d, 2)
            down = pltpu.roll(jnp.where(lane >= cz - d, before, v), d, 2)
            total = total + WEIGHTS[d] * (up + down)
        acc[s] = total + rows_sum(v, own)
        return 0

    lax.fori_loop(0, species, along_z, 0)

    def along_x(s, _):
        cells = [xl[s, i] for i in range(REACH)] + [u[s, i] for i in range(cx)]
        cells += [xr[s, i] for i in range(REACH)]
        for i in range(cx):
            total = acc[s, i]
            for d in range(1, REACH + 1):
                total = total + WEIGHTS[d] * (cells[REACH + i - d] + cells[REACH + i + d])
            acc[s, i] = total
        return 0

    def along_y(s, _):
        total = acc[s]
        for side, weights in enumerate(remote):
            total = total + rows_sum(ys[side, s], weights)
        out[s] = u[s] + (strength[s] * (1.0 / 1024.0)) * total
        return 0

    for k, (begin, size) in enumerate(spans):
        part = pl.ds(begin, size)
        for copy in x_copies[k]:
            copy.wait_recv()
        lax.fori_loop(begin, begin + size, along_x, 0)
        for copy in y_copies[k]:
            copy.wait_recv()
        lax.fori_loop(begin, begin + size, along_y, 0)
    for k in range(len(spans)):
        for copy in y_copies[k] + x_copies[k]:
            copy.wait_send()


def local(nx, ny, nz, fields, strength):
    species, cx, cy, cz = fields.shape
    cuts = CUTS if sum(CUTS) == species else (1,) * species
    pieces = len(cuts)
    sides = 1 if ny == 2 else 2
    groups = cz // SLOT
    rows_packed = -(-species // groups)
    block = (species, cx, cy, cz)
    dma = pltpu.SemaphoreType.DMA
    return pl.pallas_call(
        functools.partial(kernel, nx, ny, nz, cuts),
        out_shape=pltpu.VMEM(block, jnp.float32),
        in_specs=[pl.BlockSpec(memory_space=pltpu.HBM), pl.BlockSpec(memory_space=pl.ANY)],
        out_specs=pl.BlockSpec(memory_space=pltpu.VMEM),
        scratch_shapes=[
            pltpu.SMEM((species,), jnp.float32),
            pltpu.VMEM(block, jnp.float32),
            pltpu.VMEM(block, jnp.float32),
            pltpu.VMEM((species, REACH, cy, cz), jnp.float32),
            pltpu.VMEM((species, REACH, cy, cz), jnp.float32),
            pltpu.VMEM((sides,) + block, jnp.float32),
            pltpu.VMEM((2, rows_packed, cx, cy, cz), jnp.float32),
            pltpu.VMEM((2, rows_packed, cx, cy, cz), jnp.float32),
            dma((pieces + 1,)),
            dma((2, pieces)),
            dma((2, pieces)),
            dma((sides, pieces)),
            dma((sides, pieces)),
            dma((2,)),
            dma((2,)),
            pltpu.SemaphoreType.REGULAR((4,)),
        ],
        compiler_params=pltpu.CompilerParams(collective_id=0, has_side_effects=True, vmem_limit_bytes=56 * 1024 * 1024),
        name="filter_pass",
    )(fields, strength)


def solution(mesh):
    sizes = mesh.shape
    return jax.shard_map(
        functools.partial(local, sizes["gx"], sizes["gy"], sizes["gz"]),
        mesh=mesh,
        in_specs=(P(None, "gx", "gy", "gz"), P()),
        out_specs=P(None, "gx", "gy", "gz"),
        check_vma=False,
    )
```
